32 devices in a mesh: dp: 4 (over y, x), cls: 8 (over z, core).
Axes of the slice: x: 2, y: 2, z: 4, core: 2. Of those that a mesh axis runs over, the one named last changes fastest.
Arguments:
- embeddings: float32 [2048, 512], P('dp'), may hold values from -60 to 60, as said below
- classifier: float32 [131072, 512], P(('dp', 'cls')), may hold values from -60 to 60, as said below
- labels: int32 [2048], replicated, may hold values from 0 to 131071
- row_scale: float32 [2048], replicated, may hold values from 16 to 512
Outputs:
- loss: float32 [2048], P(('dp', 'cls'))
The draws below stay inside these ranges and needn't reach their ends.
Inputs may be any that keep to these rules, and one draw needn't show every extreme that they name: `embeddings`: rows of different scales. `classifier`: rows of different scales.
All inputs are finite; a program needn't handle non-finite values.
Results may differ from the reference program's by a relative error of at most 0.0003.
Values sent between devices are 32-bit elements; how exact they have to be, the bound alone decides.
A program may use at most 128 MiB of HBM per device.

```python
import math
import jax
import jax.numpy as jnp
from jax import lax

D = 512
CLS_DEV = 4096
EMBEDS = 2048
CLASSES = 131072


def class_row(base, index):
    row_key = jax.random.fold_in(base, index)
    return jax.random.truncated_normal(row_key, -6.0, 6.0, (D,), jnp.float32)


def many_rows(base, indices):

    def single(index):
        return class_row(base, index)
    return jax.vmap(single)(indices)


def draw_classifier(key, part):
    base = jax.random.fold_in(key, 101)
    rows = many_rows(base, jnp.arange(CLASSES, dtype=jnp.int32))
    scales = jnp.exp(jax.random.uniform(jax.random.fold_in(key, 102), (CLASSES, 1), jnp.float32, 0.0, math.log(10.0)))
    return rows * scales


def draw_embeddings(key, part):
    scales = jnp.exp(jax.random.uniform(jax.random.fold_in(key, 202), (EMBEDS, 1), jnp.float32, 0.0, math.log(10.0)))
    noise = jax.random.truncated_normal(jax.random.fold_in(key, 201), -6.0, 6.0, (EMBEDS, D), jnp.float32)
    return noise * scales


def with_ends(values, key, least, high):
    shape = values.shape
    spot = [jax.random.randint(jax.random.fold_in(key, axis), (), 0, shape[axis]) for axis in range(len(shape))]
    values = values.at[tuple(spot)].set(least)
    longest = shape.index(max(shape))
    spot[longest] = (spot[longest] + 1) % shape[longest]
    return values.at[tuple(spot)].set(high)


def setup_inputs(seed: int = 0) -> dict:
    keys = jax.random.split(jax.random.key(seed), 5)
    return {
        "embeddings": draw_embeddings(jax.random.fold_in(keys[4], 71), 0),
        "classifier": draw_classifier(jax.random.fold_in(keys[4], 71), 0),
        "labels": with_ends(jax.random.randint(keys[2], (EMBEDS,), 0, CLASSES), jax.random.fold_in(keys[2], 1), 0, CLASSES - 1).astype(jnp.int32),
        "row_scale": jnp.clip(jnp.exp(jax.random.uniform(keys[3], (EMBEDS,), jnp.float32, math.log(16.0), math.log(512.0))), 16.0, 512.0),
    }


MARGIN = 0.5
COS_MARGIN = math.cos(MARGIN)
SIN_MARGIN = math.sin(MARGIN)

def unit_rows(values):
    return values * lax.rsqrt(lax.optimization_barrier(jnp.sum(values * values, axis=-1, keepdims=True)) + 1e-06)

def margin_logit(units, picked, scales):
    cosine = lax.optimization_barrier(jnp.sum(units * picked, axis=-1))
    across = units - cosine[:, None] * picked
    sine = jnp.sqrt(lax.optimization_barrier(jnp.sum(across * across, axis=-1)))
    return scales * (cosine * COS_MARGIN - sine * SIN_MARGIN)

def block_stats(units, rows, class_ids, labels, scales, picked, owned):
    cosine = lax.dot_general(units, rows, (((1,), (1,)), ((), ())), precision=lax.Precision.HIGHEST, preferred_element_type=jnp.float32)
    target = margin_logit(units, picked, scales)
    hit = labels[:, None] == class_ids[None, :]
    logits = jnp.where(hit, target[:, None], scales[:, None] * cosine)
    peak = lax.optimization_barrier(jnp.max(logits, axis=1))
    total = lax.optimization_barrier(jnp.sum(jnp.exp(logits - peak[:, None]), axis=1))
    return (peak, total, jnp.where(owned, target, jnp.zeros_like(target)))

def merge_rows(first, second):
    peak = jnp.maximum(first[0], second[0])
    total = first[1] * jnp.exp(first[0] - peak) + second[1] * jnp.exp(second[0] - peak)
    return (peak, total, first[2] + second[2])

def reference(embeddings, classifier, labels, row_scale):
    units = unit_rows(embeddings)
    count = CLASSES // CLS_DEV
    blocks = classifier.reshape(count, CLS_DEV, D)
    numbers = jnp.arange(count).astype(jnp.int32)

    def step(carry, item):
        block, number = item
        normed = unit_rows(block)
        offset = number * CLS_DEV
        class_ids = offset + jnp.arange(CLS_DEV).astype(jnp.int32)
        owned = (labels >= offset) & (labels < offset + CLS_DEV)
        local = jnp.clip(labels - offset, 0, CLS_DEV - 1).astype(jnp.int32)
        picked = jnp.take(normed, local, axis=0)
        stats = block_stats(units, normed, class_ids, labels, row_scale, picked, owned)
        return (merge_rows(carry, stats), None)
    start = jnp.full((EMBEDS,), -1e+30, jnp.float32)
    empty = jnp.zeros((EMBEDS,), jnp.float32)
    (peak, total, target), unused = lax.scan(step, (start, empty, empty), (blocks, numbers))
    return peak + jnp.log(total) - target
```

```python
import functools
import math

import jax
import jax.numpy as jnp
from jax import lax
from jax.experimental import pallas as pl
from jax.experimental.pallas import tpu as pltpu
from jax.sharding import PartitionSpec as P

MARGIN = 0.5
COS_MARGIN = math.cos(MARGIN)
SIN_MARGIN = math.sin(MARGIN)
LOG2E = math.log2(math.e)
LN2 = math.log(2.0)
LOW = -1e30
MESH = pl.DeviceIdType.MESH


def kernel(ndp, ncls, chunk, emb_hbm, cls_hbm, lab_sm, lab_ref, scale_ref, out_ref,
           emb, raw, unit_w, picks, unit_e, buf0, buf1, stats, got,
           emb_sem, raw_sem, xs, xr, ys, yr, ds, dr, ss, sr):
    dp, cls = lax.axis_index("dp"), lax.axis_index("cls")
    core = lax.rem(cls, 2)
    ndev = ndp * ncls
    me = dp * ncls + cls
    rows, width = cls_hbm.shape
    half = width // 2
    piece = emb_hbm.shape[0] // 4
    groups, lanes = lab_ref.shape
    nchunk = rows // chunk
    offset = me * rows

    barrier = pltpu.get_barrier_semaphore()

    @pl.loop(1, ndev)
    def _(k):
        to = lax.rem(me + k, ndev)
        pl.semaphore_signal(barrier, inc=1, device_id=(to // ncls, lax.rem(to, ncls)), device_id_type=MESH)

    emb_in = [
        pltpu.make_async_copy(emb_hbm.at[:, pl.ds(c * half, half)], emb.at[0, c], emb_sem.at[c])
        for c in range(2)
    ]
    for copy in emb_in:
        copy.start()
    raw_in = [
        pltpu.make_async_copy(raw_hbm, raw.at[pl.ds(i * chunk, chunk)], raw_sem.at[i])
        for i in range(nchunk)
        for raw_hbm in [cls_hbm.at[pl.ds(i * chunk, chunk)]]
    ]
    for copy in raw_in:
        copy.start()

    def prepare(i):
        raw_in[i].wait()

        @pl.loop(0, chunk // 64)
        def _(b):
            at = pl.ds(pl.multiple_of(i * chunk + b * 64, 64), 64)
            w = raw[at, :]
            inv = lax.rsqrt(jnp.sum(w * w, axis=1, keepdims=True) + 1e-06)
            unit_w[at, :] = (w * inv).astype(jnp.bfloat16)

    early = nchunk // 2
    for i in range(early):
        prepare(i)
    for copy in emb_in:
        copy.wait()
    pl.semaphore_wait(barrier, ndev - 1)

    to_x = (dp ^ 1, cls)
    to_y = (dp ^ 2, cls)
    partner = (dp, cls ^ 1)

    def part(slot, j):
        return emb.at[slot, core, pl.ds(j * piece, piece)]

    def send(src, dst, s, r, k, to):
        copy = pltpu.make_async_remote_copy(
            src_ref=part(*src), dst_ref=part(*dst), send_sem=s.at[k], recv_sem=r.at[k],
            device_id=to, device_id_type=MESH,
        )
        copy.start()
        return copy

    x_slot = [(1, 0), (1, 1), (1, 2), (1, 3), (3, 2), (3, 3)]
    y_slot = [(2, 2), (2, 3), (2, 0), (2, 1), (3, 0), (3, 1)]
    x_copy, y_copy, d_copy = [], [], []
    for k in range(4):
        x_copy.append(send((0, x_slot[k][1]), x_slot[k], xs, xr, k, to_x))
        y_copy.append(send((0, y_slot[k][1]), y_slot[k], ys, yr, k, to_y))
    for i in range(early, nchunk):
        prepare(i)

    def forward(k):
        x_copy[k].wait_recv()
        y_copy[k].wait_recv()
        if k < 2:
            x_copy.append(send(y_slot[k], x_slot[k + 4], xs, xr, k + 4, to_x))
            y_copy.append(send(x_slot[k], y_slot[k + 4], ys, yr, k + 4, to_y))
        d_copy.append(send(x_slot[k], x_slot[k], ds, dr, 2 * k, partner))
        d_copy.append(send(y_slot[k], y_slot[k], ds, dr, 2 * k + 1, partner))

    def unit_rows(pair):
        left = jnp.concatenate([emb[s, 0, pl.ds(j * piece, piece), :] for s, j in pair], axis=0)
        right = jnp.concatenate([emb[s, 1, pl.ds(j * piece, piece), :] for s, j in pair], axis=0)
        values = jnp.concatenate([left, right], axis=1)
        return values * lax.rsqrt(jnp.sum(values * values, axis=1, keepdims=True) + 1e-06)

    def compute(pair):
        group = [(dp ^ s) * 4 + j for s, j in pair]
        unit_e[...] = unit_rows(pair).astype(jnp.bfloat16)
        local = jnp.concatenate([lab_ref[pl.ds(g, 1), :] for g in group], axis=1) - offset
        scale = jnp.concatenate([scale_ref[pl.ds(g, 1), :] for g in group], axis=1)
        scale2 = scale * LOG2E
        wide = 2 * piece
        share = wide // nchunk

        def dot(i, buf):
            at = pl.ds(pl.multiple_of(i * chunk, chunk), chunk)
            buf[...] = lax.dot_general(
                unit_w[at, :], unit_e[...], (((1,), (1,)), ((), ())),
                preferred_element_type=jnp.float32,
            )
            first = i * share
            base = jnp.where(first < piece, group[0] * piece, group[1] * piece - piece) + first
            for t in range(share):
                here = jnp.clip(lab_sm[base + t] - offset, 0, rows - 1)
                picks[pl.ds(first + t, 1), :] = raw[pl.ds(here, 1), :]

        def fold(i, buf, peak, total):
            ids = lax.broadcasted_iota(jnp.int32, (chunk, wide), 0)
            z = jnp.where(ids == local - i * chunk, LOW, buf[...] * scale2)
            z = z.reshape(chunk // 8, 8, wide)
            fresh = jnp.maximum(peak, jnp.max(z, axis=0))
            total = total * jnp.exp2(peak - fresh) + jnp.sum(jnp.exp2(z - fresh[None]), axis=0)
            return fresh, total

        dot(0, buf0)

        def both(h, carry):
            i = 2 * h
            dot(i + 1, buf1)
            carry = fold(i, buf0, *carry)
            dot(i + 2, buf0)
            return fold(i + 1, buf1, *carry)

        start = (jnp.full((8, wide), LOW, jnp.float32), jnp.zeros((8, wide), jnp.float32))
        carry = lax.fori_loop(0, nchunk // 2 - 1, both, start)
        dot(nchunk - 1, buf1)
        carry = fold(nchunk - 2, buf0, *carry)
        peak, total = fold(nchunk - 1, buf1, *carry)
        best = jnp.max(peak, axis=0, keepdims=True)
        total = jnp.sum(total * jnp.exp2(peak - best), axis=0, keepdims=True)

        units = unit_rows(pair)
        picked = picks[...]
        picked = picked * lax.rsqrt(jnp.sum(picked * picked, axis=1, keepdims=True) + 1e-06)
        cosine = jnp.sum(units * picked, axis=1, keepdims=True)
        across = units - cosine * picked
        sine = jnp.sqrt(jnp.sum(across * across, axis=1, keepdims=True))
        target = cosine * COS_MARGIN - sine * SIN_MARGIN
        target = jnp.transpose(jnp.broadcast_to(target, (wide, 128)))[0:1, :]
        owned = (local >= 0) & (local < rows)
        target = jnp.where(owned, scale * target, 0.0)
        for n, g in enumerate(group):
            cut = slice(n * piece, (n + 1) * piece)
            stats[pl.ds(g, 1), 0:1, :] = best[:, cut][None]
            stats[pl.ds(g, 1), 1:2, :] = total[:, cut][None]
            stats[pl.ds(g, 1), 2:3, :] = target[:, cut][None]

    def compute_stage(k):
        d_copy[2 * k].wait_recv()
        d_copy[2 * k + 1].wait_recv()
        compute([x_slot[k], y_slot[k]])

    compute([(0, 0), (0, 1)])
    forward(0)
    compute([(0, 2), (0, 3)])
    for k in range(5):
        forward(k + 1)
        compute_stage(k)
    compute_stage(5)

    share = groups * lanes // ndev
    per = lanes // share

    def outgoing(k):
        to = lax.rem(me + k, ndev)
        return pltpu.make_async_remote_copy(
            src_ref=stats.at[to // per], dst_ref=got.at[k], send_sem=ss, recv_sem=sr,
            device_id=(to // ncls, lax.rem(to, ncls)), device_id_type=MESH,
        )

    @pl.loop(1, ndev)
    def _(k):
        outgoing(k).start()

    got[0] = stats[me // per]
    for copy in x_copy + y_copy + d_copy:
        copy.wait_send()
    rest = got.at[pl.ds(1, ndev - 1)]
    pltpu.make_async_copy(rest, rest, ss).wait()
    pltpu.make_async_copy(rest, rest, sr).wait()

    everyone = got[...]
    peaks, totals = everyone[:, 0, :], everyone[:, 1, :]
    target = jnp.sum(everyone[:, 2, :], axis=0, keepdims=True)
    best = jnp.maximum(jnp.max(peaks, axis=0, keepdims=True), target * LOG2E)
    total = jnp.sum(totals * jnp.exp2(peaks - best), axis=0, keepdims=True) + jnp.exp2(target * LOG2E - best)
    loss = best * LN2 + jnp.log(total) - target
    mine = loss[:, 0:share]
    for q in range(1, per):
        mine = jnp.where(lax.rem(me, per) == q, loss[:, q * share:(q + 1) * share], mine)
    out_ref[...] = mine


def body(embeddings, classifier, labels, row_scale):
    ndp, ncls = lax.axis_size("dp"), lax.axis_size("cls")
    assert ndp == 4 and ncls % 2 == 0
    ndev = ndp * ncls
    block, width = embeddings.shape
    rows = classifier.shape[0]
    count = labels.shape[0]
    piece = block // 4
    chunk = rows // 8
    groups = count // piece
    f32 = jnp.float32
    any_spec = pl.BlockSpec(memory_space=pl.ANY)
    vmem = pl.BlockSpec(memory_space=pltpu.VMEM)
    dma = pltpu.SemaphoreType.DMA
    out = pl.pallas_call(
        functools.partial(kernel, ndp, ncls, chunk),
        out_shape=jax.ShapeDtypeStruct((1, count // ndev), f32),
        in_specs=[any_spec, any_spec, pl.BlockSpec(memory_space=pltpu.SMEM), vmem, vmem],
        out_specs=vmem,
        scratch_shapes=[
            pltpu.VMEM((4, 2, block, width // 2), f32),
            pltpu.VMEM((rows, width), f32),
            pltpu.VMEM((rows, width), jnp.bfloat16),
            pltpu.VMEM((2 * piece, width), f32),
            pltpu.VMEM((2 * piece, width), jnp.bfloat16),
            pltpu.VMEM((chunk, 2 * piece), f32),
            pltpu.VMEM((chunk, 2 * piece), f32),
            pltpu.VMEM((groups, 8, piece), f32),
            pltpu.VMEM((ndev, 8, piece), f32),
            dma((2,)), dma((8,)), dma((6,)), dma((6,)), dma((6,)), dma((6,)),
            dma((12,)), dma((12,)), dma, dma,
        ],
        compiler_params=pltpu.CompilerParams(
            collective_id=0, has_side_effects=True, vmem_limit_bytes=56 * 1024 * 1024
        ),
    )(embeddings, classifier, labels, labels.reshape(groups, piece), row_scale.reshape(groups, piece))
    return out.reshape(count // ndev)


def solution(mesh):
    placed = (P("dp", None), P(("dp", "cls"), None), P(), P())
    return jax.shard_map(
        body, mesh=mesh, in_specs=placed, out_specs=P(("dp", "cls")), check_vma=False
    )
```
